512 devices in a mesh: clips: 2 (over y), tm: 8 (over x), rows: 32 (over z, core).
Axes of the slice: x: 8, y: 2, z: 16, core: 2. Of those that a mesh axis runs over, the one named last changes fastest.
The devices are a block of a 8x8x16 slice.
Arguments:
- features: bfloat16 [128, 128, 32, 192], P(('clips', 'tm'), 'rows'), parts along dimension 0, may hold values from -6 to 6
- norm_gain: float32 [192], replicated, may hold values from 0.1 to 1.9
- conv_weight: bfloat16 [3, 3, 3, 192, 96], replicated, may hold values from -0.078125 to 0.078125
- out_grad: bfloat16 [128, 128, 32, 96], P(('clips', 'tm'), 'rows'), parts along dimension 0, may hold values from -6 to 6
Outputs:
- grad_features: bfloat16 [128, 128, 32, 192], P(('clips', 'tm'), 'rows'), parts along dimension 0
- grad_weight: float32 [6, 3, 3, 192, 96], P('clips'), parts along dimension 0
The draws below stay inside these ranges and needn't reach their ends.
There are 2 independent parts, one for each index of `clips`. The reference program is written for one: setup_inputs(seed, part) draws one part's arguments, and reference() takes and returns one part's arrays. A program takes and returns all parts, laid end to end along the dimension named above; an argument that names none is the same for every part. Nothing has to cross between parts.
All inputs are finite; a program needn't handle non-finite values.
Results may differ from the reference program's by a relative error of at most 0.0029.
Values may be sent and summed in bfloat16 or wider, within the bound.
No kernel may reach another device: no remote copies, remote signals or barrier semaphores. Data moves between devices by JAX's collectives and lax.ppermute only.
A program may use at most 64 MiB of HBM per device.

```python
import jax
import jax.numpy as jnp
from jax import lax

CIN = 192
COUT = 96
WIDTH = 32
FRAMES = 64
ROWS = 128
POSITIONS = 262144


def block_scale(stream_key, extent, split, least, high):
    factor_of, own = 1.0, jax.random.fold_in(stream_key, 6)
    for position, parts in split:
        draws = jnp.exp(jax.random.uniform(jax.random.fold_in(own, position), (parts,), jnp.float32, least / len(split), high / len(split)))
        factor_of = factor_of * jnp.repeat(draws, extent[position] // parts).reshape([-1 if axis == position else 1 for axis in range(len(extent))])
    return factor_of


def normal_values(stream_key, dims, scale, most, shards=(), dtype=jnp.bfloat16):
    values = scale * jax.random.normal(stream_key, dims, jnp.float32)
    if shards:
        values = values * block_scale(stream_key, dims, shards, -0.22, 0.18)
    return jnp.clip(values, -most, most).astype(dtype)


def setup_inputs(seed: int = 0, part: int = 0) -> dict:
    seeds = jax.random.split(jax.random.key(seed), 5)
    own_keys = jax.random.split(jax.random.fold_in(seeds[4], part), 5)
    features = normal_values(own_keys[0], (FRAMES, ROWS, WIDTH, CIN), 1.0, 6.0, ((0, 8), (1, 32)))
    norm_gain = jnp.clip(1.0 + 0.18 * jax.random.normal(seeds[1], (CIN,), jnp.float32), 0.1, 1.9)
    conv_weight = normal_values(seeds[2], (3, 3, 3, CIN, COUT), (27 * CIN) ** -0.5, 0.078125)
    out_grad = normal_values(own_keys[3], (FRAMES, ROWS, WIDTH, COUT), 1.0, 6.0, ((0, 8), (1, 32)))
    return dict(features=features, norm_gain=norm_gain, conv_weight=conv_weight, out_grad=out_grad)


def activate(features, norm_gain):
    values = features.astype(jnp.float32)
    inv_rms = lax.rsqrt(lax.optimization_barrier(jnp.mean(values * values, axis=-1, keepdims=True)) + 1e-06)
    unit = values * inv_rms
    normed = unit * norm_gain
    return (normed, inv_rms, unit)

def reference(features, norm_gain, conv_weight, out_grad):
    normed, inv_rms, unit = activate(features, norm_gain)
    act = jax.nn.silu(normed).astype(jnp.bfloat16)
    frames, height, width = (act.shape[0], act.shape[1], act.shape[2])
    act_pad = jnp.pad(act, ((2, 0), (1, 1), (1, 1), (0, 0)))
    out_pad = jnp.pad(out_grad, ((0, 2), (1, 1), (1, 1), (0, 0)))
    count = frames * height * width
    grad_act = jnp.zeros((count, CIN), jnp.float32)
    kernel_terms = []
    flat_out = out_grad.reshape(count, COUT)
    for i in range(3):
        for j in range(3):
            for k in range(3):
                shifted = out_pad[2 - i:2 - i + frames, 2 - j:2 - j + height, 2 - k:2 - k + width].reshape(count, COUT)
                grad_act = grad_act + jnp.dot(shifted, conv_weight[i, j, k].T, preferred_element_type=jnp.float32)
                window = act_pad[i:i + frames, j:j + height, k:k + width].reshape(count, CIN)
                kernel_terms.append(jnp.dot(window.T, flat_out, preferred_element_type=jnp.float32))
    grad_weight = jnp.stack(kernel_terms).reshape(3, 3, 3, CIN, COUT) * (1.0 / jnp.sqrt(jnp.float32(POSITIONS)))
    grad_act = grad_act.reshape(frames, height, width, CIN)
    sigma = jax.nn.sigmoid(normed)
    grad_normed = grad_act * sigma * (1.0 + normed * (1.0 - sigma))
    grad_unit = grad_normed * norm_gain
    grad_features = inv_rms * (grad_unit - unit * lax.optimization_barrier(jnp.mean(grad_unit * unit, axis=-1, keepdims=True)))
    return (grad_features.astype(jnp.bfloat16), grad_weight)
```

```python
import functools

import jax
import jax.numpy as jnp
from jax import lax
from jax.experimental import pallas as pl
from jax.experimental.pallas import tpu as pltpu
from jax.sharding import Mesh
from jax.sharding import PartitionSpec as P

NEAR = 2
ROWS = ("far", "near", "core")
LANES = 128
SUBLANES = 8
GRANT = pltpu.CompilerParams(vmem_limit_bytes=20 * 2**20)


def vmem():
    return pl.BlockSpec(memory_space=pltpu.VMEM)


def smem():
    return pl.BlockSpec(memory_space=pltpu.SMEM)


def anywhere():
    return pl.BlockSpec(memory_space=pl.ANY)


def cost(flops, moved):
    return pl.CostEstimate(flops=flops, bytes_accessed=moved, transcendentals=0)


def normalised(values, gain):
    inv_rms = lax.rsqrt(jnp.mean(values * values, axis=-1, keepdims=True) + 1e-06)
    unit = values * inv_rms
    return unit * gain, inv_rms, unit


def act_kernel(features_ref, gain_ref, act_ref):
    normed, _, _ = normalised(features_ref[...].astype(jnp.float32), gain_ref[...])
    act = normed / (1.0 + jnp.exp(-normed))
    act_ref[...] = act.T.astype(jnp.bfloat16)


def column_taps(block):
    block = block.astype(jnp.float32)
    axis = block.ndim - 2
    width = block.shape[axis]
    column = lax.broadcasted_iota(jnp.int32, block.shape, axis)
    later = jnp.where(column == width - 1, 0.0, pltpu.roll(block, width - 1, axis))
    sooner = jnp.where(column == 0, 0.0, pltpu.roll(block, 1, axis))
    return jnp.concatenate([later, block, sooner], axis=-1).astype(jnp.bfloat16)


def tap_plan():
    return 4, 2


def tile_plan(rows, columns):
    full, rest = divmod(columns, LANES)
    strips = rows // SUBLANES
    per_tile = LANES // rest if rest else 1
    extra = -(-strips // per_tile) if rest else 0
    return full, rest, strips, per_tile, extra


def kernel_grad_kernel(
    core_ref,
    mine_ref,
    theirs_ref,
    outer_ref,
    outer_theirs_ref,
    act_ref,
    act_theirs_ref,
    out_ref,
    taps_ref,
    terms_ref,
):
    core = core_ref[0]
    other = 1 - core
    frames, height = mine_ref.shape[:2]

    def build(row, carry):
        taps_ref[:, core * height + row + 1] = column_taps(mine_ref[:, row])
        taps_ref[:, other * height + row + 1] = column_taps(theirs_ref[:, row])
        return carry

    lax.fori_loop(0, height, build, 0)
    taps_ref[:, core * (2 * height + 1)] = column_taps(outer_ref[:, 0])
    taps_ref[:, other * (2 * height + 1)] = column_taps(outer_theirs_ref[:, 0])
    act = act_ref[...]
    act_theirs = act_theirs_ref[...]
    lanes = taps_ref.shape[3]
    third = lanes // 3
    positions = act.shape[1]
    pairs, middle = tap_plan()

    def pair(i, j):
        total = None
        for left, place in ((act, core), (act_theirs, other)):
            shifted = taps_ref[pl.ds(2 - i, frames - 2), pl.ds(place * height + 2 - j, height)]
            term = jnp.dot(
                left, shifted.reshape(positions, lanes), preferred_element_type=jnp.float32
            )
            total = term if total is None else total + term
        return total

    for n in range(pairs):
        p = core * (pairs + 1) + n
        terms_ref[:, n * lanes : (n + 1) * lanes] = pair(p // 3, p % 3)
    centre = pair(1, 1)
    terms_ref[:, pairs * lanes : pairs * lanes + middle * third] = jnp.where(
        core == 0, centre[:, : middle * third], centre[:, lanes - middle * third :]
    )

    groups, packed, _ = out_ref.shape
    rows = act.shape[0] // groups
    full, rest, strips, per_tile, extra = tile_plan(rows, terms_ref.shape[1])
    zeros = jnp.zeros((SUBLANES, LANES), jnp.float32)
    for g in range(groups):

        def strip(s, span):
            at = g * rows + s * SUBLANES
            return terms_ref[at : at + SUBLANES, span]

        tiles = [
            strip(s, slice(t * LANES, (t + 1) * LANES)) for s in range(strips) for t in range(full)
        ]
        for e in range(extra):
            ends = [
                strip(s, slice(full * LANES, full * LANES + rest))
                for s in range(e * per_tile, min((e + 1) * per_tile, strips))
            ]
            used = rest * len(ends)
            if used < LANES:
                ends.append(zeros[:, used:])
            tiles.append(jnp.concatenate(ends, axis=-1))
        tiles += [zeros] * (packed // SUBLANES - len(tiles))
        out_ref[g] = jnp.concatenate(tiles, axis=0).astype(jnp.bfloat16)


def features_kernel(
    core_ref,
    mine_ref,
    theirs_ref,
    outer_ref,
    features_ref,
    gain_ref,
    weight_ref,
    after_ref,
    out_ref,
    taps_ref,
    turned_ref,
):
    core = core_ref[0]
    frames, height, width, outputs = mine_ref.shape
    last = height - 1

    def build(row, carry):
        taps_ref[:, row + 1] = column_taps(mine_ref[:, row])
        return carry

    lax.fori_loop(0, height, build, 0)
    taps_ref[:, core * (height + 1)] = column_taps(outer_ref[:, 0])
    taps_ref[:, (1 - core) * (height + 1)] = column_taps(theirs_ref[:, core * last])

    def turn(n, carry):
        for k in range(3):
            turned = weight_ref[n * 3 + k].astype(jnp.float32).T
            turned_ref[n, k * outputs : (k + 1) * outputs] = turned.astype(jnp.bfloat16)
        return carry

    lax.fori_loop(0, 9, turn, 0)
    gain = gain_ref[...]
    lanes = taps_ref.shape[3]
    step = 2
    count = step * height * width

    def piece(n, carry):
        grad_act = None
        for i in range(3):
            for j in range(3):
                shifted = taps_ref[pl.ds(n * step + 2 - i, step), 2 - j : 2 - j + height]
                term = jnp.dot(
                    shifted.reshape(count, lanes),
                    turned_ref[i * 3 + j],
                    preferred_element_type=jnp.float32,
                )
                grad_act = term if grad_act is None else grad_act + term
        rows = pl.ds(n * count, count)
        normed, inv_rms, unit = normalised(features_ref[rows].astype(jnp.float32), gain)
        sigma = 1.0 / (1.0 + jnp.exp(-normed))
        grad_unit = grad_act * sigma * (1.0 + normed * (1.0 - sigma)) * gain
        mean = jnp.mean(grad_unit * unit, axis=-1, keepdims=True)
        out_ref[rows] = (inv_rms * (grad_unit - unit * mean)).astype(jnp.bfloat16)
        return carry

    lax.fori_loop(0, (frames - 2) // step, piece, 0)


def sum_first_kernel(blocks_ref, after_ref, out_ref):
    total = blocks_ref[0].astype(jnp.float32)
    for p in range(1, blocks_ref.shape[0]):
        total = total + blocks_ref[p].astype(jnp.float32)
    out_ref[...] = total


def sum_last_kernel(scale, blocks_ref, out_ref):
    total = blocks_ref[0]
    for p in range(1, blocks_ref.shape[0]):
        total = total + blocks_ref[p]
    total = (total * scale).astype(jnp.bfloat16)
    for p in range(out_ref.shape[0]):
        out_ref[p] = total


def assemble_kernel(rows, columns, core_ref, mine_ref, theirs_ref, out_ref, whole_ref, sem):
    core = core_ref[0]
    full, rest, strips, per_tile, extra = tile_plan(rows, columns)
    outputs = out_ref.shape[2]
    taps = columns // outputs
    pairs, middle = tap_plan()
    copies = []
    for g in range(mine_ref.shape[0]):
        for ref, owner in ((mine_ref, core), (theirs_ref, 1 - core)):
            block = ref[g].astype(jnp.float32)

            def tile(n):
                return block[n * SUBLANES : (n + 1) * SUBLANES]

            spans = [
                jnp.concatenate([tile(s * full + t) for s in range(strips)], axis=0)
                for t in range(full)
            ]
            if rest:
                ends = []
                for s in range(strips):
                    at = (s % per_tile) * rest
                    ends.append(tile(strips * full + s // per_tile)[:, at : at + rest])
                spans.append(jnp.concatenate(ends, axis=0))
            for t in range(taps):
                if t < 3 * pairs:
                    at = t + owner * (3 * (pairs + 1))
                elif t < taps - 1:
                    at = t + owner * 2
                else:
                    at = t + owner
                begin, end = t * outputs, (t + 1) * outputs
                parts = []
                while begin < end:
                    n, low = divmod(begin, LANES)
                    high = min(LANES, low + end - begin)
                    parts.append(spans[n][:, low:high])
                    begin += high - low
                whole_ref[at, g * rows : (g + 1) * rows] = jnp.concatenate(parts, axis=-1)
        here = pl.ds(g * rows, rows)
        copies.append(pltpu.make_async_copy(whole_ref.at[:, here], out_ref.at[:, here], sem.at[g]))
        copies[-1].start()
    for copy in copies:
        copy.wait()


def exchange(blocks, axis):
    return lax.all_to_all(blocks, axis, 0, 0, tiled=True)


def on_device(features, norm_gain, conv_weight, out_grad):
    frames, height, width, channels = features.shape
    outputs = out_grad.shape[3]
    count = frames * height * width
    groups, far, near, cores = (lax.axis_size(a) for a in ("tm", *ROWS))
    chips = far * near
    core = lax.axis_index("core")
    core_arg = core.astype(jnp.int32).reshape(1)
    swap = [(0, 1), (1, 0)]

    after = lax.ppermute(out_grad[:2], "tm", [(g + 1, g) for g in range(groups - 1)])
    mine = jnp.concatenate([out_grad, after], axis=0)
    edge = jnp.where(core == 0, mine[:, :1], mine[:, height - 1 :])
    across = [(2 * z + 1, 2 * z + 2) for z in range(chips - 1)]
    across += [(b, a) for a, b in across]
    along = [(2 * z + 1, 2 * z + 3) for z in range(chips - 1)]
    along += [(2 * z + 2, 2 * z) for z in range(chips - 1)]
    outer = lax.ppermute(edge, ROWS, across)
    outer_theirs = lax.ppermute(edge, ROWS, along)
    theirs = lax.ppermute(mine, "core", swap)

    flat = features.reshape(count, channels)
    gain = norm_gain.reshape(1, channels)
    act = pl.pallas_call(
        act_kernel,
        out_shape=jax.ShapeDtypeStruct((channels, count), jnp.bfloat16),
        in_specs=[vmem(), vmem()],
        out_specs=vmem(),
        cost_estimate=cost(count * channels * 20, count * channels * 4),
        compiler_params=GRANT,
        name="act",
    )(flat, gain)
    act_theirs = lax.ppermute(act, "core", swap)

    pairs, middle = tap_plan()
    taps = 3 * pairs + middle
    columns = taps * outputs
    rows = channels // groups
    full, _, strips, _, extra = tile_plan(rows, columns)
    share = -(-(full * strips + extra) // chips) * SUBLANES
    terms = pl.pallas_call(
        kernel_grad_kernel,
        out_shape=jax.ShapeDtypeStruct((groups, chips * share, LANES), jnp.bfloat16),
        in_specs=[smem()] + [vmem()] * 6,
        out_specs=vmem(),
        scratch_shapes=[
            pltpu.VMEM((frames + 2, 2 * (height + 1), width, 3 * outputs), jnp.bfloat16),
            pltpu.VMEM((channels, columns), jnp.float32),
        ],
        cost_estimate=cost(2 * 2 * count * channels * columns, 2 * channels * columns),
        compiler_params=GRANT,
        name="kernel_grad",
    )(core_arg, mine, theirs, outer, outer_theirs, act, act_theirs)

    grad_features = pl.pallas_call(
        features_kernel,
        out_shape=jax.ShapeDtypeStruct((count, channels), jnp.bfloat16),
        in_specs=[smem()] + [vmem()] * 6 + [anywhere()],
        out_specs=vmem(),
        scratch_shapes=[
            pltpu.VMEM((frames + 2, height + 2, width, 3 * outputs), jnp.bfloat16),
            pltpu.VMEM((9, 3 * outputs, channels), jnp.bfloat16),
        ],
        cost_estimate=cost(2 * count * channels * 27 * outputs, 2 * 27 * channels * outputs),
        compiler_params=GRANT,
        name="grad_features",
    )(
        core_arg,
        mine,
        theirs,
        outer,
        flat,
        gain,
        conv_weight.reshape(27, channels, outputs),
        terms,
    )

    first = ("tm", "near")
    received = exchange(terms.reshape(groups * near, far * share, LANES), first)
    summed = pl.pallas_call(
        sum_first_kernel,
        out_shape=jax.ShapeDtypeStruct((far * share, LANES), jnp.float32),
        in_specs=[vmem(), anywhere()],
        out_specs=vmem(),
        cost_estimate=cost(count * channels, 2 * channels * columns),
        compiler_params=GRANT,
        name="sum_first",
    )(received, grad_features)
    received = exchange(summed.reshape(far, share, LANES), "far")
    positions = count * groups * chips * cores
    scale = float(positions) ** -0.5
    total = pl.pallas_call(
        functools.partial(sum_last_kernel, scale),
        out_shape=jax.ShapeDtypeStruct((far, share, LANES), jnp.bfloat16),
        in_specs=[vmem()],
        out_specs=vmem(),
        cost_estimate=cost(count * channels, 8 * far * share * LANES),
        compiler_params=GRANT,
        name="sum_last",
    )(received)
    gathered = exchange(total, "far").reshape(1, far * share, LANES)
    gathered = jnp.broadcast_to(gathered, (groups * near, far * share, LANES))
    gathered = exchange(gathered, first).reshape(groups, chips * share, LANES)
    gathered_theirs = lax.ppermute(gathered, "core", swap)
    grad_weight = pl.pallas_call(
        functools.partial(assemble_kernel, rows, columns),
        out_shape=jax.ShapeDtypeStruct((27, channels, outputs), jnp.float32),
        in_specs=[smem(), vmem(), vmem()],
        out_specs=anywhere(),
        scratch_shapes=[
            pltpu.VMEM((27, channels, outputs), jnp.float32),
            pltpu.SemaphoreType.DMA((groups,)),
        ],
        cost_estimate=cost(27 * channels * outputs * 8, 8 * 27 * channels * outputs),
        compiler_params=GRANT,
        name="assemble",
    )(core_arg, gathered, gathered_theirs)
    return (
        grad_features.reshape(features.shape),
        grad_weight.reshape(3, 3, 3, channels, outputs),
    )


def solution(mesh):
    clips, groups, lines = (mesh.shape[a] for a in ("clips", "tm", "rows"))
    torus = Mesh(
        mesh.devices.reshape(clips, groups, lines // (2 * NEAR), NEAR, 2), ("clips", "tm", *ROWS)
    )
    in_specs = (
        P(("clips", "tm"), ROWS, None, None),
        P(),
        P(),
        P(("clips", "tm"), ROWS, None, None),
    )
    out_specs = (P(("clips", "tm"), ROWS, None, None), P("clips", None, None, None, None))
    return jax.shard_map(
        on_device, mesh=torus, in_specs=in_specs, out_specs=out_specs, check_vma=False
    )
```

```python
import functools

import jax
import jax.numpy as jnp
from jax import lax
from jax.experimental import pallas as pl
from jax.experimental.pallas import tpu as pltpu
from jax.sharding import Mesh
from jax.sharding import PartitionSpec as P

NEAR = 4
ONE_STAGE = True
ROWS = ("far", "near", "core")
LANES = 128
SUBLANES = 8
GRANT = pltpu.CompilerParams(vmem_limit_bytes=20 * 2**20)


def vmem():
    return pl.BlockSpec(memory_space=pltpu.VMEM)


def smem():
    return pl.BlockSpec(memory_space=pltpu.SMEM)


def anywhere():
    return pl.BlockSpec(memory_space=pl.ANY)


def cost(flops, moved):
    return pl.CostEstimate(flops=flops, bytes_accessed=moved, transcendentals=0)


def normalised(values, gain):
    inv_rms = lax.rsqrt(jnp.mean(values * values, axis=-1, keepdims=True) + 1e-06)
    unit = values * inv_rms
    return unit * gain, inv_rms, unit


def prepare_kernel(features_ref, gain_ref, out_grad_ref, act_ref, rows_ref):
    normed, _, _ = normalised(features_ref[...].astype(jnp.float32), gain_ref[...])
    act = (normed / (1.0 + jnp.exp(-normed))).T.astype(jnp.bfloat16)
    frames = act_ref.shape[0]
    positions = act.shape[1] // frames
    for t in range(frames):
        act_ref[t] = act[:, t * positions : (t + 1) * positions]
    for r in range(rows_ref.shape[0]):
        rows_ref[r] = out_grad_ref[:, r]


def edge_kernel(core_ref, rows_ref, after_ref, edge_ref):
    row = core_ref[0] * (rows_ref.shape[0] - 1)
    frames = rows_ref.shape[1]
    edge_ref[:frames] = rows_ref[row]
    edge_ref[frames:] = after_ref[:, row]


def packet_plan(frames, channels, width):
    per_frame = channels // width
    return per_frame, per_frame * frames


def merge_kernel(act_ref, rows_ref, after_ref, outer_ref, packet_ref):
    frames, channels, lanes = act_ref.shape
    height, _, width, outputs = rows_ref.shape
    _, first = packet_plan(frames, channels, width)
    later = after_ref.shape[0]
    packet_ref[:first] = act_ref[...].reshape(first, width, lanes)
    for r in range(height):
        at = first + r * (frames + later)
        packet_ref[at : at + frames, :, :outputs] = rows_ref[r]
        packet_ref[at + frames : at + frames + later, :, :outputs] = after_ref[:, r]
    at = first + height * (frames + later)
    packet_ref[at : at + frames + later, :, :outputs] = outer_ref[...]


def packet_act(packet_ref, frames, channels):
    width, lanes = packet_ref.shape[1:]
    per_frame, first = packet_plan(frames, channels, width)
    blocks = [
        packet_ref[t * per_frame : (t + 1) * per_frame].reshape(channels, lanes)
        for t in range(frames)
    ]
    return jnp.concatenate(blocks, axis=-1)


def packet_row(packet_ref, row, frames, channels, outputs):
    width = packet_ref.shape[1]
    _, first = packet_plan(frames, channels, width)
    return packet_ref[pl.ds(first + row * (frames + 2), frames + 2), :, :outputs]


def column_taps(block):
    block = block.astype(jnp.float32)
    axis = block.ndim - 2
    width = block.shape[axis]
    column = lax.broadcasted_iota(jnp.int32, block.shape, axis)
    later = jnp.where(column == width - 1, 0.0, pltpu.roll(block, width - 1, axis))
    sooner = jnp.where(column == 0, 0.0, pltpu.roll(block, 1, axis))
    return jnp.concatenate([later, block, sooner], axis=-1).astype(jnp.bfloat16)


def tap_plan():
    return 4, 2


def tile_plan(rows, columns):
    full, rest = divmod(columns, LANES)
    strips = rows // SUBLANES
    per_tile = LANES // rest if rest else 1
    extra = -(-strips // per_tile) if rest else 0
    return full, rest, strips, per_tile, extra


def kernel_grad_kernel(
    core_ref,
    mine_ref,
    theirs_ref,
    out_ref,
    inner_ref,
    taps_ref,
    terms_ref,
):
    core = core_ref[0]
    other = 1 - core
    frames = taps_ref.shape[0]
    height = taps_ref.shape[1] // 2 - 1
    channels = terms_ref.shape[0]
    outputs = inner_ref.shape[2]
    inner_ref[...] = packet_row(theirs_ref, core * (height - 1), frames - 2, channels, outputs)

    def build(row, carry):
        for ref, place in ((mine_ref, core), (theirs_ref, other)):
            block = packet_row(ref, row, frames - 2, channels, outputs)
            taps_ref[:, place * height + row + 1] = column_taps(block)
        return carry

    lax.fori_loop(0, height, build, 0)
    for ref, place in ((mine_ref, core), (theirs_ref, other)):
        block = packet_row(ref, height, frames - 2, channels, outputs)
        taps_ref[:, place * (2 * height + 1)] = column_taps(block)
    act = packet_act(mine_ref, frames - 2, channels)
    act_theirs = packet_act(theirs_ref, frames - 2, channels)
    lanes = taps_ref.shape[3]
    third = lanes // 3
    positions = act.shape[1]
    pairs, middle = tap_plan()

    def pair(i, j):
        total = None
        for left, place in ((act, core), (act_theirs, other)):
            shifted = taps_ref[pl.ds(2 - i, frames - 2), pl.ds(place * height + 2 - j, height)]
            term = jnp.dot(
                left, shifted.reshape(positions, lanes), preferred_element_type=jnp.float32
            )
            total = term if total is None else total + term
        return total

    for n in range(pairs):
        p = core * (pairs + 1) + n
        terms_ref[:, n * lanes : (n + 1) * lanes] = pair(p // 3, p % 3)
    centre = pair(1, 1)
    terms_ref[:, pairs * lanes : pairs * lanes + middle * third] = jnp.where(
        core == 0, centre[:, : middle * third], centre[:, lanes - middle * third :]
    )

    groups, packed, _ = out_ref.shape
    rows = act.shape[0] // groups
    full, rest, strips, per_tile, extra = tile_plan(rows, terms_ref.shape[1])
    zeros = jnp.zeros((SUBLANES, LANES), jnp.float32)
    for g in range(groups):

        def strip(s, span):
            at = g * rows + s * SUBLANES
            return terms_ref[at : at + SUBLANES, span]

        tiles = [
            strip(s, slice(t * LANES, (t + 1) * LANES)) for s in range(strips) for t in range(full)
        ]
        for e in range(extra):
            ends = [
                strip(s, slice(full * LANES, full * LANES + rest))
                for s in range(e * per_tile, min((e + 1) * per_tile, strips))
            ]
            used = rest * len(ends)
            if used < LANES:
                ends.append(zeros[:, used:])
            tiles.append(jnp.concatenate(ends, axis=-1))
        tiles += [zeros] * (packed // SUBLANES - len(tiles))
        out_ref[g] = jnp.concatenate(tiles, axis=0).astype(jnp.bfloat16)


def features_kernel(
    core_ref,
    mine_ref,
    inner_ref,
    features_ref,
    gain_ref,
    weight_ref,
    out_ref,
    token_ref,
    taps_ref,
    turned_ref,
):
    core = core_ref[0]
    frames, height, width = taps_ref.shape[:3]
    height = height - 2
    outputs = inner_ref.shape[2]
    channels = features_ref.shape[1]
    token_ref[...] = jnp.zeros_like(token_ref)

    def row_of(ref, row):
        return column_taps(packet_row(ref, row, frames - 2, channels, outputs))

    def build(row, carry):
        taps_ref[:, row + 1] = row_of(mine_ref, row)
        return carry

    lax.fori_loop(0, height, build, 0)
    taps_ref[:, core * (height + 1)] = row_of(mine_ref, height)
    taps_ref[:, (1 - core) * (height + 1)] = column_taps(inner_ref[...])

    def turn(n, carry):
        for k in range(3):
            turned = weight_ref[n * 3 + k].astype(jnp.float32).T
            turned_ref[n, k * outputs : (k + 1) * outputs] = turned.astype(jnp.bfloat16)
        return carry

    lax.fori_loop(0, 9, turn, 0)
    gain = gain_ref[...]
    lanes = taps_ref.shape[3]
    step = 2
    count = step * height * width

    def piece(n, carry):
        grad_act = None
        for i in range(3):
            for j in range(3):
                shifted = taps_ref[pl.ds(n * step + 2 - i, step), 2 - j : 2 - j + height]
                term = jnp.dot(
                    shifted.reshape(count, lanes),
                    turned_ref[i * 3 + j],
                    preferred_element_type=jnp.float32,
                )
                grad_act = term if grad_act is None else grad_act + term
        rows = pl.ds(n * count, count)
        normed, inv_rms, unit = normalised(features_ref[rows].astype(jnp.float32), gain)
        sigma = 1.0 / (1.0 + jnp.exp(-normed))
        grad_unit = grad_act * sigma * (1.0 + normed * (1.0 - sigma)) * gain
        mean = jnp.mean(grad_unit * unit, axis=-1, keepdims=True)
        out_ref[rows] = (inv_rms * (grad_unit - unit * mean)).astype(jnp.bfloat16)
        return carry

    lax.fori_loop(0, (frames - 2) // step, piece, 0)


def sum_first_kernel(blocks_ref, after_ref, out_ref):
    total = blocks_ref[0].astype(jnp.float32)
    for p in range(1, blocks_ref.shape[0]):
        total = total + blocks_ref[p].astype(jnp.float32)
    if len(out_ref.shape) == 2:
        out_ref[...] = total
    else:
        for p in range(out_ref.shape[0]):
            out_ref[p] = total


def sum_last_kernel(scale, blocks_ref, out_ref):
    total = blocks_ref[0]
    for p in range(1, blocks_ref.shape[0]):
        total = total + blocks_ref[p]
    total = (total * scale).astype(jnp.bfloat16)
    for p in range(out_ref.shape[0]):
        out_ref[p] = total


def assemble_kernel(rows, columns, core_ref, mine_ref, theirs_ref, out_ref, whole_ref, sem):
    core = core_ref[0]
    full, rest, strips, per_tile, extra = tile_plan(rows, columns)
    outputs = out_ref.shape[2]
    taps = columns // outputs
    pairs, middle = tap_plan()
    copies = []
    for g in range(mine_ref.shape[0]):
        for ref, owner in ((mine_ref, core), (theirs_ref, 1 - core)):
            block = ref[g].astype(jnp.float32)

            def tile(n):
                return block[n * SUBLANES : (n + 1) * SUBLANES]

            spans = [
                jnp.concatenate([tile(s * full + t) for s in range(strips)], axis=0)
                for t in range(full)
            ]
            if rest:
                ends = []
                for s in range(strips):
                    at = (s % per_tile) * rest
                    ends.append(tile(strips * full + s // per_tile)[:, at : at + rest])
                spans.append(jnp.concatenate(ends, axis=0))
            for t in range(taps):
                if t < 3 * pairs:
                    at = t + owner * (3 * (pairs + 1))
                elif t < taps - 1:
                    at = t + owner * 2
                else:
                    at = t + owner
                begin, end = t * outputs, (t + 1) * outputs
                parts = []
                while begin < end:
                    n, low = divmod(begin, LANES)
                    high = min(LANES, low + end - begin)
                    parts.append(spans[n][:, low:high])
                    begin += high - low
                whole_ref[at, g * rows : (g + 1) * rows] = jnp.concatenate(parts, axis=-1)
        here = pl.ds(g * rows, rows)
        copies.append(pltpu.make_async_copy(whole_ref.at[:, here], out_ref.at[:, here], sem.at[g]))
        copies[-1].start()
    for copy in copies:
        copy.wait()


def exchange(blocks, axis):
    return lax.all_to_all(blocks, axis, 0, 0, tiled=True)


def on_device(features, norm_gain, conv_weight, out_grad):
    frames, height, width, channels = features.shape
    outputs = out_grad.shape[3]
    count = frames * height * width
    groups, far, near, cores = (lax.axis_size(a) for a in ("tm", *ROWS))
    chips = far * near
    core = lax.axis_index("core")
    core_arg = core.astype(jnp.int32).reshape(1)
    swap = [(0, 1), (1, 0)]

    after = lax.ppermute(out_grad[:2], "tm", [(g + 1, g) for g in range(groups - 1)])
    flat = features.reshape(count, channels)
    gain = norm_gain.reshape(1, channels)
    act, rows_own = pl.pallas_call(
        prepare_kernel,
        out_shape=(
            jax.ShapeDtypeStruct((frames, channels, height * width), jnp.bfloat16),
            jax.ShapeDtypeStruct((height, frames, width, outputs), jnp.bfloat16),
        ),
        in_specs=[vmem()] * 3,
        out_specs=(vmem(), vmem()),
        cost_estimate=cost(count * channels * 20, count * channels * 4),
        compiler_params=GRANT,
        name="prepare",
    )(flat, gain, out_grad)
    row_shape = jax.ShapeDtypeStruct((frames + 2, width, outputs), jnp.bfloat16)
    edge = pl.pallas_call(
        edge_kernel,
        out_shape=row_shape,
        in_specs=[smem(), vmem(), vmem()],
        out_specs=vmem(),
        cost_estimate=cost(1000, frames * width * outputs * 4),
        compiler_params=GRANT,
        name="edge",
    )(core_arg, rows_own, after)
    across = [(2 * z + 1, 2 * z + 2) for z in range(chips - 1)]
    across += [(b, a) for a, b in across]
    outer = lax.ppermute(edge, ROWS, across)
    _, first_row = packet_plan(frames, channels, width)
    length = first_row + (frames + 2) * (height + 1)
    packet = pl.pallas_call(
        merge_kernel,
        out_shape=jax.ShapeDtypeStruct((length, width, LANES), jnp.bfloat16),
        in_specs=[vmem()] * 4,
        out_specs=vmem(),
        cost_estimate=cost(1000, count * channels * 4),
        compiler_params=GRANT,
        name="merge",
    )(act, rows_own, after, outer)
    theirs = lax.ppermute(packet, "core", swap)

    pairs, middle = tap_plan()
    taps = 3 * pairs + middle
    columns = taps * outputs
    rows = channels // groups
    full, _, strips, _, extra = tile_plan(rows, columns)
    share = -(-(full * strips + extra) // chips) * SUBLANES
    token = jax.ShapeDtypeStruct((SUBLANES, LANES), jnp.float32)
    terms, inner = pl.pallas_call(
        kernel_grad_kernel,
        out_shape=(
            jax.ShapeDtypeStruct((groups, chips * share, LANES), jnp.bfloat16),
            row_shape,
        ),
        in_specs=[smem()] + [vmem()] * 2,
        out_specs=(vmem(), vmem()),
        scratch_shapes=[
            pltpu.VMEM((frames + 2, 2 * (height + 1), width, 3 * outputs), jnp.bfloat16),
            pltpu.VMEM((channels, columns), jnp.float32),
        ],
        cost_estimate=cost(2 * 2 * count * channels * columns, 2 * channels * columns),
        compiler_params=GRANT,
        name="kernel_grad",
    )(core_arg, packet, theirs)

    grad_features, features_done = pl.pallas_call(
        features_kernel,
        out_shape=(jax.ShapeDtypeStruct((count, channels), jnp.bfloat16), token),
        in_specs=[smem()] + [vmem()] * 5,
        out_specs=(vmem(), vmem()),
        scratch_shapes=[
            pltpu.VMEM((frames + 2, height + 2, width, 3 * outputs), jnp.bfloat16),
            pltpu.VMEM((9, 3 * outputs, channels), jnp.bfloat16),
        ],
        cost_estimate=cost(2 * count * channels * 27 * outputs, 2 * 27 * channels * outputs),
        compiler_params=GRANT,
        name="grad_features",
    )(
        core_arg,
        packet,
        inner,
        flat,
        gain,
        conv_weight.reshape(27, channels, outputs),
    )

    first = ("tm", "near")
    peers = groups * near
    block = far * share
    received = exchange(terms.reshape(peers, block, LANES), first)
    summed = pl.pallas_call(
        sum_first_kernel,
        out_shape=jax.ShapeDtypeStruct(
            (far, block, LANES) if ONE_STAGE else (block, LANES), jnp.float32
        ),
        in_specs=[vmem(), anywhere()],
        out_specs=vmem(),
        cost_estimate=cost(count * channels, 2 * channels * columns),
        compiler_params=GRANT,
        name="sum_first",
    )(received, features_done)
    part = block if ONE_STAGE else share
    received = exchange(summed.reshape(far, part, LANES), "far")
    positions = count * groups * chips * cores
    scale = float(positions) ** -0.5
    total = pl.pallas_call(
        functools.partial(sum_last_kernel, scale),
        out_shape=jax.ShapeDtypeStruct((peers if ONE_STAGE else far, part, LANES), jnp.bfloat16),
        in_specs=[vmem()],
        out_specs=vmem(),
        cost_estimate=cost(count * channels, 8 * far * part * LANES),
        compiler_params=GRANT,
        name="sum_last",
    )(received)
    if not ONE_STAGE:
        gathered = exchange(total, "far").reshape(1, block, LANES)
        total = jnp.broadcast_to(gathered, (peers, block, LANES))
    gathered = exchange(total, first).reshape(groups, chips * share, LANES)
    gathered_theirs = lax.ppermute(gathered, "core", swap)
    grad_weight = pl.pallas_call(
        functools.partial(assemble_kernel, rows, columns),
        out_shape=jax.ShapeDtypeStruct((27, channels, outputs), jnp.float32),
        in_specs=[smem(), vmem(), vmem()],
        out_specs=anywhere(),
        scratch_shapes=[
            pltpu.VMEM((27, channels, outputs), jnp.float32),
            pltpu.SemaphoreType.DMA((groups,)),
        ],
        cost_estimate=cost(27 * channels * outputs * 8, 8 * 27 * channels * outputs),
        compiler_params=GRANT,
        name="assemble",
    )(core_arg, gathered, gathered_theirs)
    return (
        grad_features.reshape(features.shape),
        grad_weight.reshape(3, 3, 3, channels, outputs),
    )


def solution(mesh):
    clips, groups, lines = (mesh.shape[a] for a in ("clips", "tm", "rows"))
    torus = Mesh(
        mesh.devices.reshape(clips, groups, lines // (2 * NEAR), NEAR, 2), ("clips", "tm", *ROWS)
    )
    in_specs = (
        P(("clips", "tm"), ROWS, None, None),
        P(),
        P(),
        P(("clips", "tm"), ROWS, None, None),
    )
    out_specs = (P(("clips", "tm"), ROWS, None, None), P("clips", None, None, None, None))
    return jax.shard_map(
        on_device, mesh=torus, in_specs=in_specs, out_specs=out_specs, check_vma=False
    )
```

```python
import functools

import jax
import jax.numpy as jnp
from jax import lax
from jax.experimental import pallas as pl
from jax.experimental.pallas import tpu as pltpu
from jax.sharding import Mesh
from jax.sharding import PartitionSpec as P

NEAR = 4
ONE_STAGE = True
ROWS = ("far", "near", "core")
LANES = 128
SUBLANES = 8
GRANT = pltpu.CompilerParams(vmem_limit_bytes=20 * 2**20)


def vmem():
    return pl.BlockSpec(memory_space=pltpu.VMEM)


def smem():
    return pl.BlockSpec(memory_space=pltpu.SMEM)


def anywhere():
    return pl.BlockSpec(memory_space=pl.ANY)


def cost(flops, moved):
    return pl.CostEstimate(flops=flops, bytes_accessed=moved, transcendentals=0)


def normalised(values, gain):
    inv_rms = lax.rsqrt(jnp.mean(values * values, axis=-1, keepdims=True) + 1e-06)
    unit = values * inv_rms
    return unit * gain, inv_rms, unit


def split_kernel(core_ref, out_grad_ref, rows_ref, head_ref, edge_ref, corner_ref):
    height = rows_ref.shape[0]
    later = head_ref.shape[0]
    for r in range(height):
        rows_ref[r] = out_grad_ref[:, r]
    head_ref[...] = out_grad_ref[:later]
    row = core_ref[0] * (height - 1)
    edge_ref[...] = out_grad_ref[:, row]
    corner_ref[...] = out_grad_ref[:later, row]


def act_kernel(features_ref, gain_ref, act_ref):
    normed, _, _ = normalised(features_ref[...].astype(jnp.float32), gain_ref[...])
    act = (normed / (1.0 + jnp.exp(-normed))).T.astype(jnp.bfloat16)
    frames = act_ref.shape[0]
    positions = act.shape[1] // frames
    for t in range(frames):
        act_ref[t] = act[:, t * positions : (t + 1) * positions]


def packet_plan(frames, channels, width):
    per_frame = channels // width
    return per_frame, per_frame * frames


def merge_kernel(act_ref, rows_ref, after_ref, outer_ref, corner_ref, packet_ref):
    frames, channels, lanes = act_ref.shape
    height, _, width, outputs = rows_ref.shape
    _, first = packet_plan(frames, channels, width)
    later = after_ref.shape[0]
    packet_ref[:first] = act_ref[...].reshape(first, width, lanes)
    for r in range(height):
        at = first + r * (frames + later)
        packet_ref[at : at + frames, :, :outputs] = rows_ref[r]
        packet_ref[at + frames : at + frames + later, :, :outputs] = after_ref[:, r]
    at = first + height * (frames + later)
    packet_ref[at : at + frames, :, :outputs] = outer_ref[...]
    packet_ref[at + frames : at + frames + later, :, :outputs] = corner_ref[...]


def packet_act(packet_ref, frames, channels):
    width, lanes = packet_ref.shape[1:]
    per_frame, first = packet_plan(frames, channels, width)
    blocks = [
        packet_ref[t * per_frame : (t + 1) * per_frame].reshape(channels, lanes)
        for t in range(frames)
    ]
    return jnp.concatenate(blocks, axis=-1)


def packet_row(packet_ref, row, frames, channels, outputs):
    width = packet_ref.shape[1]
    _, first = packet_plan(frames, channels, width)
    return packet_ref[pl.ds(first + row * (frames + 2), frames + 2), :, :outputs]


def column_taps(block):
    block = block.astype(jnp.float32)
    axis = block.ndim - 2
    width = block.shape[axis]
    column = lax.broadcasted_iota(jnp.int32, block.shape, axis)
    later = jnp.where(column == width - 1, 0.0, pltpu.roll(block, width - 1, axis))
    sooner = jnp.where(column == 0, 0.0, pltpu.roll(block, 1, axis))
    return jnp.concatenate([later, block, sooner], axis=-1).astype(jnp.bfloat16)


def tap_plan():
    return 4, 2


def tile_plan(rows, columns):
    full, rest = divmod(columns, LANES)
    strips = rows // SUBLANES
    per_tile = LANES // rest if rest else 1
    extra = -(-strips // per_tile) if rest else 0
    return full, rest, strips, per_tile, extra


def kernel_grad_kernel(
    core_ref,
    mine_ref,
    theirs_ref,
    out_ref,
    inner_ref,
    taps_ref,
    terms_ref,
    shift_ref,
):
    core = core_ref[0]
    other = 1 - core
    frames = taps_ref.shape[0]
    height = taps_ref.shape[1] // 2 - 1
    channels = terms_ref.shape[0]
    outputs = inner_ref.shape[2]
    inner_ref[...] = packet_row(theirs_ref, core * (height - 1), frames - 2, channels, outputs)

    width = taps_ref.shape[2]
    pad = SUBLANES
    shift_ref[:, :pad] = jnp.zeros_like(shift_ref[:, :pad])
    shift_ref[:, pad + width :] = jnp.zeros_like(shift_ref[:, pad + width :])
    _, first = packet_plan(frames - 2, channels, width)

    def place_row(ref, row, slot):
        block = ref[pl.ds(first + row * frames, frames)]
        shift_ref[:, pad : pad + width] = block.astype(jnp.float32)
        taps_ref[:, slot, :, :LANES] = shift_ref[:, pad + 1 : pad + 1 + width].astype(jnp.bfloat16)
        taps_ref[:, slot, :, LANES : 2 * LANES] = block
        taps_ref[:, slot, :, 2 * LANES :] = shift_ref[:, pad - 1 : pad - 1 + width].astype(
            jnp.bfloat16
        )

    for ref, place in ((mine_ref, core), (theirs_ref, other)):
        for row in range(height):
            place_row(ref, row, place * height + row + 1)
        place_row(ref, height, place * (2 * height + 1))
    act = packet_act(mine_ref, frames - 2, channels)
    act_theirs = packet_act(theirs_ref, frames - 2, channels)
    lanes = taps_ref.shape[3]
    positions = act.shape[1]
    pairs, middle = tap_plan()

    def pair(i, j):
        total = None
        for left, place in ((act, core), (act_theirs, other)):
            shifted = taps_ref[pl.ds(2 - i, frames - 2), pl.ds(place * height + 2 - j, height)]
            term = jnp.dot(
                left, shifted.reshape(positions, lanes), preferred_element_type=jnp.float32
            )
            total = term if total is None else total + term
        return total

    def keep(tap, total, k):
        terms_ref[:, tap * outputs : (tap + 1) * outputs] = total[:, k * LANES : k * LANES + outputs]

    for n in range(pairs):
        p = core * (pairs + 1) + n
        total = pair(p // 3, p % 3)
        for k in range(3):
            keep(3 * n + k, total, k)
    centre = pair(1, 1)
    centre = jnp.where(
        core == 0, centre[:, : middle * LANES], centre[:, lanes - middle * LANES :]
    )
    for k in range(middle):
        keep(3 * pairs + k, centre, k)

    groups, packed, _ = out_ref.shape
    rows = act.shape[0] // groups
    full, rest, strips, per_tile, extra = tile_plan(rows, terms_ref.shape[1])
    zeros = jnp.zeros((SUBLANES, LANES), jnp.float32)
    for g in range(groups):

        def strip(s, span):
            at = g * rows + s * SUBLANES
            return terms_ref[at : at + SUBLANES, span]

        tiles = [
            strip(s, slice(t * LANES, (t + 1) * LANES)) for s in range(strips) for t in range(full)
        ]
        for e in range(extra):
            ends = [
                strip(s, slice(full * LANES, full * LANES + rest))
                for s in range(e * per_tile, min((e + 1) * per_tile, strips))
            ]
            used = rest * len(ends)
            if used < LANES:
                ends.append(zeros[:, used:])
            tiles.append(jnp.concatenate(ends, axis=-1))
        tiles += [zeros] * (packed // SUBLANES - len(tiles))
        out_ref[g] = jnp.concatenate(tiles, axis=0).astype(jnp.bfloat16)


def features_kernel(
    core_ref,
    mine_ref,
    inner_ref,
    features_ref,
    gain_ref,
    weight_ref,
    out_ref,
    token_ref,
    taps_ref,
    turned_ref,
):
    core = core_ref[0]
    frames, height, width = taps_ref.shape[:3]
    height = height - 2
    outputs = inner_ref.shape[2]
    channels = features_ref.shape[1]
    token_ref[...] = jnp.zeros_like(token_ref)

    def row_of(ref, row):
        return column_taps(packet_row(ref, row, frames - 2, channels, outputs))

    def build(row, carry):
        taps_ref[:, row + 1] = row_of(mine_ref, row)
        return carry

    lax.fori_loop(0, height, build, 0)
    taps_ref[:, core * (height + 1)] = row_of(mine_ref, height)
    taps_ref[:, (1 - core) * (height + 1)] = column_taps(inner_ref[...])

    def turn(n, carry):
        for k in range(3):
            turned = weight_ref[n * 3 + k].astype(jnp.float32).T
            turned_ref[n, k * outputs : (k + 1) * outputs] = turned.astype(jnp.bfloat16)
        return carry

    lax.fori_loop(0, 9, turn, 0)
    gain = gain_ref[...]
    lanes = taps_ref.shape[3]
    step = 2
    count = step * height * width

    def piece(n, carry):
        grad_act = None
        for i in range(3):
            for j in range(3):
                shifted = taps_ref[pl.ds(n * step + 2 - i, step), 2 - j : 2 - j + height]
                term = jnp.dot(
                    shifted.reshape(count, lanes),
                    turned_ref[i * 3 + j],
                    preferred_element_type=jnp.float32,
                )
                grad_act = term if grad_act is None else grad_act + term
        rows = pl.ds(n * count, count)
        normed, inv_rms, unit = normalised(features_ref[rows].astype(jnp.float32), gain)
        sigma = 1.0 / (1.0 + jnp.exp(-normed))
        grad_unit = grad_act * sigma * (1.0 + normed * (1.0 - sigma)) * gain
        mean = jnp.mean(grad_unit * unit, axis=-1, keepdims=True)
        out_ref[rows] = (inv_rms * (grad_unit - unit * mean)).astype(jnp.bfloat16)
        return carry

    lax.fori_loop(0, (frames - 2) // step, piece, 0)


def sum_first_kernel(blocks_ref, after_ref, out_ref):
    total = blocks_ref[0].astype(jnp.float32)
    for p in range(1, blocks_ref.shape[0]):
        total = total + blocks_ref[p].astype(jnp.float32)
    if len(out_ref.shape) == 2:
        out_ref[...] = total
    else:
        for p in range(out_ref.shape[0]):
            out_ref[p] = total


def sum_last_kernel(scale, blocks_ref, out_ref):
    total = blocks_ref[0]
    for p in range(1, blocks_ref.shape[0]):
        total = total + blocks_ref[p]
    total = (total * scale).astype(jnp.bfloat16)
    for p in range(out_ref.shape[0]):
        out_ref[p] = total


def assemble_kernel(rows, columns, core_ref, mine_ref, theirs_ref, out_ref, whole_ref, sem):
    core = core_ref[0]
    full, rest, strips, per_tile, extra = tile_plan(rows, columns)
    outputs = out_ref.shape[2]
    taps = columns // outputs
    pairs, middle = tap_plan()
    copies = []
    for g in range(mine_ref.shape[0]):
        for ref, owner in ((mine_ref, core), (theirs_ref, 1 - core)):
            block = ref[g].astype(jnp.float32)

            def tile(n):
                return block[n * SUBLANES : (n + 1) * SUBLANES]

            spans = [
                jnp.concatenate([tile(s * full + t) for s in range(strips)], axis=0)
                for t in range(full)
            ]
            if rest:
                ends = []
                for s in range(strips):
                    at = (s % per_tile) * rest
                    ends.append(tile(strips * full + s // per_tile)[:, at : at + rest])
                spans.append(jnp.concatenate(ends, axis=0))
            for t in range(taps):
                if t < 3 * pairs:
                    at = t + owner * (3 * (pairs + 1))
                elif t < taps - 1:
                    at = t + owner * 2
                else:
                    at = t + owner
                begin, end = t * outputs, (t + 1) * outputs
                parts = []
                while begin < end:
                    n, low = divmod(begin, LANES)
                    high = min(LANES, low + end - begin)
                    parts.append(spans[n][:, low:high])
                    begin += high - low
                whole_ref[at, g * rows : (g + 1) * rows] = jnp.concatenate(parts, axis=-1)
        here = pl.ds(g * rows, rows)
        copies.append(pltpu.make_async_copy(whole_ref.at[:, here], out_ref.at[:, here], sem.at[g]))
        copies[-1].start()
    for copy in copies:
        copy.wait()


def exchange(blocks, axis):
    return lax.all_to_all(blocks, axis, 0, 0, tiled=True)


def on_device(features, norm_gain, conv_weight, out_grad):
    frames, height, width, channels = features.shape
    outputs = out_grad.shape[3]
    count = frames * height * width
    groups, far, near, cores = (lax.axis_size(a) for a in ("tm", *ROWS))
    chips = far * near
    core = lax.axis_index("core")
    core_arg = core.astype(jnp.int32).reshape(1)
    swap = [(0, 1), (1, 0)]

    later = 2
    block_of = functools.partial(jax.ShapeDtypeStruct, dtype=jnp.bfloat16)
    rows_own, head, edge, corner = pl.pallas_call(
        split_kernel,
        out_shape=(
            block_of((height, frames, width, outputs)),
            block_of((later, height, width, outputs)),
            block_of((frames, width, outputs)),
            block_of((later, width, outputs)),
        ),
        in_specs=[smem(), vmem()],
        out_specs=(vmem(),) * 4,
        cost_estimate=cost(1000, count * outputs * 4),
        compiler_params=GRANT,
        name="split",
    )(core_arg, out_grad)
    across = [(2 * z + 1, 2 * z + 2) for z in range(chips - 1)]
    across += [(b, a) for a, b in across]
    lines = 2 * chips
    slanted = [
        ((g + 1) * lines + a, g * lines + b) for g in range(groups - 1) for a, b in across
    ]
    after = lax.ppermute(head, "tm", [(g + 1, g) for g in range(groups - 1)])
    outer = lax.ppermute(edge, ROWS, across)
    outer_after = lax.ppermute(corner, ("tm", *ROWS), slanted)
    flat = features.reshape(count, channels)
    gain = norm_gain.reshape(1, channels)
    act = pl.pallas_call(
        act_kernel,
        out_shape=block_of((frames, channels, height * width)),
        in_specs=[vmem()] * 2,
        out_specs=vmem(),
        cost_estimate=cost(count * channels * 20, count * channels * 4),
        compiler_params=GRANT,
        name="act",
    )(flat, gain)
    _, first_row = packet_plan(frames, channels, width)
    length = first_row + (frames + later) * (height + 1)
    packet = pl.pallas_call(
        merge_kernel,
        out_shape=jax.ShapeDtypeStruct((length, width, LANES), jnp.bfloat16),
        in_specs=[vmem()] * 5,
        out_specs=vmem(),
        cost_estimate=cost(1000, count * channels * 4),
        compiler_params=GRANT,
        name="merge",
    )(act, rows_own, after, outer, outer_after)
    theirs = lax.ppermute(packet, "core", swap)

    pairs, middle = tap_plan()
    taps = 3 * pairs + middle
    columns = taps * outputs
    rows = channels // groups
    full, _, strips, _, extra = tile_plan(rows, columns)
    share = -(-(full * strips + extra) // chips) * SUBLANES
    token = jax.ShapeDtypeStruct((SUBLANES, LANES), jnp.float32)
    terms, inner = pl.pallas_call(
        kernel_grad_kernel,
        out_shape=(
            jax.ShapeDtypeStruct((groups, chips * share, LANES), jnp.bfloat16),
            block_of((frames + later, width, outputs)),
        ),
        in_specs=[smem()] + [vmem()] * 2,
        out_specs=(vmem(), vmem()),
        scratch_shapes=[
            pltpu.VMEM((frames + 2, 2 * (height + 1), width, 3 * LANES), jnp.bfloat16),
            pltpu.VMEM((channels, columns), jnp.float32),
            pltpu.VMEM((frames + 2, width + 2 * SUBLANES, LANES), jnp.float32),
        ],
        cost_estimate=cost(2 * 2 * count * channels * columns, 2 * channels * columns),
        compiler_params=GRANT,
        name="kernel_grad",
    )(core_arg, packet, theirs)

    grad_features, features_done = pl.pallas_call(
        features_kernel,
        out_shape=(jax.ShapeDtypeStruct((count, channels), jnp.bfloat16), token),
        in_specs=[smem()] + [vmem()] * 5,
        out_specs=(vmem(), vmem()),
        scratch_shapes=[
            pltpu.VMEM((frames + 2, height + 2, width, 3 * outputs), jnp.bfloat16),
            pltpu.VMEM((9, 3 * outputs, channels), jnp.bfloat16),
        ],
        cost_estimate=cost(2 * count * channels * 27 * outputs, 2 * 27 * channels * outputs),
        compiler_params=GRANT,
        name="grad_features",
    )(
        core_arg,
        packet,
        inner,
        flat,
        gain,
        conv_weight.reshape(27, channels, outputs),
    )

    first = ("tm", "near")
    peers = groups * near
    block = far * share
    received = exchange(terms.reshape(peers, block, LANES), first)
    summed = pl.pallas_call(
        sum_first_kernel,
        out_shape=jax.ShapeDtypeStruct(
            (far, block, LANES) if ONE_STAGE else (block, LANES), jnp.float32
        ),
        in_specs=[vmem(), anywhere()],
        out_specs=vmem(),
        cost_estimate=cost(count * channels, 2 * channels * columns),
        compiler_params=GRANT,
        name="sum_first",
    )(received, features_done)
    part = block if ONE_STAGE else share
    received = exchange(summed.reshape(far, part, LANES), "far")
    positions = count * groups * chips * cores
    scale = float(positions) ** -0.5
    total = pl.pallas_call(
        functools.partial(sum_last_kernel, scale),
        out_shape=jax.ShapeDtypeStruct((peers if ONE_STAGE else far, part, LANES), jnp.bfloat16),
        in_specs=[vmem()],
        out_specs=vmem(),
        cost_estimate=cost(count * channels, 8 * far * part * LANES),
        compiler_params=GRANT,
        name="sum_last",
    )(received)
    if not ONE_STAGE:
        gathered = exchange(total, "far").reshape(1, block, LANES)
        total = jnp.broadcast_to(gathered, (peers, block, LANES))
    gathered = exchange(total, first).reshape(groups, chips * share, LANES)
    gathered_theirs = lax.ppermute(gathered, "core", swap)
    grad_weight = pl.pallas_call(
        functools.partial(assemble_kernel, rows, columns),
        out_shape=jax.ShapeDtypeStruct((27, channels, outputs), jnp.float32),
        in_specs=[smem(), vmem(), vmem()],
        out_specs=anywhere(),
        scratch_shapes=[
            pltpu.VMEM((27, channels, outputs), jnp.float32),
            pltpu.SemaphoreType.DMA((groups,)),
        ],
        cost_estimate=cost(27 * channels * outputs * 8, 8 * 27 * channels * outputs),
        compiler_params=GRANT,
        name="assemble",
    )(core_arg, gathered, gathered_theirs)
    return (
        grad_features.reshape(features.shape),
        grad_weight.reshape(3, 3, 3, channels, outputs),
    )


def solution(mesh):
    clips, groups, lines = (mesh.shape[a] for a in ("clips", "tm", "rows"))
    torus = Mesh(
        mesh.devices.reshape(clips, groups, lines // (2 * NEAR), NEAR, 2), ("clips", "tm", *ROWS)
    )
    in_specs = (
        P(("clips", "tm"), ROWS, None, None),
        P(),
        P(),
        P(("clips", "tm"), ROWS, None, None),
    )
    out_specs = (P(("clips", "tm"), ROWS, None, None), P("clips", None, None, None, None))
    return jax.shard_map(
        on_device, mesh=torus, in_specs=in_specs, out_specs=out_specs, check_vma=False
    )
```

```python
import functools

import jax
import jax.numpy as jnp
from jax import lax
from jax.experimental import pallas as pl
from jax.experimental.pallas import tpu as pltpu
from jax.sharding import Mesh
from jax.sharding import PartitionSpec as P

NEAR = 4
ONE_STAGE = True
ROWS = ("far", "near", "core")
LANES = 128
SUBLANES = 8
GRANT = pltpu.CompilerParams(vmem_limit_bytes=20 * 2**20)


def vmem():
    return pl.BlockSpec(memory_space=pltpu.VMEM)


def smem():
    return pl.BlockSpec(memory_space=pltpu.SMEM)


def anywhere():
    return pl.BlockSpec(memory_space=pl.ANY)


def cost(flops, moved):
    return pl.CostEstimate(flops=flops, bytes_accessed=moved, transcendentals=0)


def normalised(values, gain):
    inv_rms = lax.rsqrt(jnp.mean(values * values, axis=-1, keepdims=True) + 1e-06)
    unit = values * inv_rms
    return unit * gain, inv_rms, unit


def split_kernel(
    core_ref,
    out_grad_hbm,
    features_hbm,
    gain_hbm,
    rows_ref,
    head_ref,
    edge_ref,
    corner_ref,
    act_ref,
    out_grad_ref,
    features_ref,
    gain_ref,
    sem,
):
    fetches = [
        pltpu.make_async_copy(source, target, sem.at[n])
        for n, (source, target) in enumerate(
            (
                (out_grad_hbm, out_grad_ref),
                (features_hbm, features_ref),
                (gain_hbm, gain_ref),
            )
        )
    ]
    for fetch in fetches:
        fetch.start()
    fetches[0].wait()
    height = rows_ref.shape[0]
    later = head_ref.shape[0]
    for r in range(height):
        rows_ref[r] = out_grad_ref[:, r]
    head_ref[...] = out_grad_ref[:later]
    row = core_ref[0] * (height - 1)
    edge_ref[...] = out_grad_ref[:, row]
    corner_ref[...] = out_grad_ref[:later, row]
    fetches[1].wait()
    fetches[2].wait()
    normed, _, _ = normalised(features_ref[...].astype(jnp.float32), gain_ref[...])
    act = (normed / (1.0 + jnp.exp(-normed))).T.astype(jnp.bfloat16)
    frames = act_ref.shape[0]
    positions = act.shape[1] // frames
    for t in range(frames):
        act_ref[t] = act[:, t * positions : (t + 1) * positions]


def packet_plan(frames, channels, width):
    per_frame = channels // width
    return per_frame, per_frame * frames


def merge_kernel(act_ref, rows_ref, after_ref, outer_ref, corner_ref, packet_ref):
    frames, channels, lanes = act_ref.shape
    height, _, width, outputs = rows_ref.shape
    _, first = packet_plan(frames, channels, width)
    later = after_ref.shape[0]
    packet_ref[:first] = act_ref[...].reshape(first, width, lanes)
    for r in range(height):
        at = first + r * (frames + later)
        packet_ref[at : at + frames, :, :outputs] = rows_ref[r]
        packet_ref[at + frames : at + frames + later, :, :outputs] = after_ref[:, r]
    at = first + height * (frames + later)
    packet_ref[at : at + frames, :, :outputs] = outer_ref[...]
    packet_ref[at + frames : at + frames + later, :, :outputs] = corner_ref[...]


def packet_act(packet_ref, frames, channels):
    width, lanes = packet_ref.shape[1:]
    per_frame, first = packet_plan(frames, channels, width)
    blocks = [
        packet_ref[t * per_frame : (t + 1) * per_frame].reshape(channels, lanes)
        for t in range(frames)
    ]
    return jnp.concatenate(blocks, axis=-1)


def packet_row(packet_ref, row, frames, channels, outputs):
    width = packet_ref.shape[1]
    _, first = packet_plan(frames, channels, width)
    return packet_ref[pl.ds(first + row * (frames + 2), frames + 2), :, :outputs]


def column_taps(block):
    block = block.astype(jnp.float32)
    axis = block.ndim - 2
    width = block.shape[axis]
    column = lax.broadcasted_iota(jnp.int32, block.shape, axis)
    later = jnp.where(column == width - 1, 0.0, pltpu.roll(block, width - 1, axis))
    sooner = jnp.where(column == 0, 0.0, pltpu.roll(block, 1, axis))
    return jnp.concatenate([later, block, sooner], axis=-1).astype(jnp.bfloat16)


def tap_plan():
    return 4, 2


def tile_plan(rows, columns):
    full, rest = divmod(columns, LANES)
    strips = rows // SUBLANES
    per_tile = LANES // rest if rest else 1
    extra = -(-strips // per_tile) if rest else 0
    return full, rest, strips, per_tile, extra


def kernel_grad_kernel(
    core_ref,
    mine_ref,
    theirs_ref,
    out_ref,
    inner_ref,
    taps_ref,
    terms_ref,
    shift_ref,
):
    core = core_ref[0]
    other = 1 - core
    frames = taps_ref.shape[0]
    height = taps_ref.shape[1] // 2 - 1
    channels = terms_ref.shape[0]
    outputs = inner_ref.shape[2]
    inner_ref[...] = packet_row(theirs_ref, core * (height - 1), frames - 2, channels, outputs)

    width = taps_ref.shape[2]
    pad = SUBLANES
    shift_ref[:, :pad] = jnp.zeros_like(shift_ref[:, :pad])
    shift_ref[:, pad + width :] = jnp.zeros_like(shift_ref[:, pad + width :])
    _, first = packet_plan(frames - 2, channels, width)

    def place_row(ref, row, slot):
        block = ref[pl.ds(first + row * frames, frames)]
        shift_ref[:, pad : pad + width] = block.astype(jnp.float32)
        taps_ref[:, slot, :, :LANES] = shift_ref[:, pad + 1 : pad + 1 + width].astype(jnp.bfloat16)
        taps_ref[:, slot, :, LANES : 2 * LANES] = block
        taps_ref[:, slot, :, 2 * LANES :] = shift_ref[:, pad - 1 : pad - 1 + width].astype(
            jnp.bfloat16
        )

    for ref, place in ((mine_ref, core), (theirs_ref, other)):
        for row in range(height):
            place_row(ref, row, place * height + row + 1)
        place_row(ref, height, place * (2 * height + 1))
    act = packet_act(mine_ref, frames - 2, channels)
    act_theirs = packet_act(theirs_ref, frames - 2, channels)
    lanes = taps_ref.shape[3]
    positions = act.shape[1]
    pairs, middle = tap_plan()

    def pair(i, j):
        total = None
        for left, place in ((act, core), (act_theirs, other)):
            shifted = taps_ref[pl.ds(2 - i, frames - 2), pl.ds(place * height + 2 - j, height)]
            term = jnp.dot(
                left, shifted.reshape(positions, lanes), preferred_element_type=jnp.float32
            )
            total = term if total is None else total + term
        return total

    def keep(tap, total, k):
        terms_ref[:, tap * outputs : (tap + 1) * outputs] = total[:, k * LANES : k * LANES + outputs]

    for n in range(pairs):
        p = core * (pairs + 1) + n
        total = pair(p // 3, p % 3)
        for k in range(3):
            keep(3 * n + k, total, k)
    centre = pair(1, 1)
    centre = jnp.where(
        core == 0, centre[:, : middle * LANES], centre[:, lanes - middle * LANES :]
    )
    for k in range(middle):
        keep(3 * pairs + k, centre, k)

    groups, packed, _ = out_ref.shape
    rows = act.shape[0] // groups
    full, rest, strips, per_tile, extra = tile_plan(rows, terms_ref.shape[1])
    zeros = jnp.zeros((SUBLANES, LANES), jnp.float32)
    for g in range(groups):

        def strip(s, span):
            at = g * rows + s * SUBLANES
            return terms_ref[at : at + SUBLANES, span]

        tiles = [
            strip(s, slice(t * LANES, (t + 1) * LANES)) for s in range(strips) for t in range(full)
        ]
        for e in range(extra):
            ends = [
                strip(s, slice(full * LANES, full * LANES + rest))
                for s in range(e * per_tile, min((e + 1) * per_tile, strips))
            ]
            used = rest * len(ends)
            if used < LANES:
                ends.append(zeros[:, used:])
            tiles.append(jnp.concatenate(ends, axis=-1))
        tiles += [zeros] * (packed // SUBLANES - len(tiles))
        out_ref[g] = jnp.concatenate(tiles, axis=0).astype(jnp.bfloat16)


def features_kernel(
    core_ref,
    mine_ref,
    inner_ref,
    features_ref,
    gain_ref,
    weight_ref,
    out_ref,
    token_ref,
    taps_ref,
    turned_ref,
):
    core = core_ref[0]
    frames, height, width = taps_ref.shape[:3]
    height = height - 2
    outputs = inner_ref.shape[2]
    channels = features_ref.shape[1]
    token_ref[...] = jnp.zeros_like(token_ref)

    def row_of(ref, row):
        return column_taps(packet_row(ref, row, frames - 2, channels, outputs))

    def build(row, carry):
        taps_ref[:, row + 1] = row_of(mine_ref, row)
        return carry

    lax.fori_loop(0, height, build, 0)
    taps_ref[:, core * (height + 1)] = row_of(mine_ref, height)
    taps_ref[:, (1 - core) * (height + 1)] = column_taps(inner_ref[...])

    def turn(n, carry):
        for k in range(3):
            turned = weight_ref[n * 3 + k].astype(jnp.float32).T
            turned_ref[n, k * outputs : (k + 1) * outputs] = turned.astype(jnp.bfloat16)
        return carry

    lax.fori_loop(0, 9, turn, 0)
    gain = gain_ref[...]
    lanes = taps_ref.shape[3]
    step = 2
    count = step * height * width

    def piece(n, carry):
        grad_act = None
        for i in range(3):
            for j in range(3):
                shifted = taps_ref[pl.ds(n * step + 2 - i, step), 2 - j : 2 - j + height]
                term = jnp.dot(
                    shifted.reshape(count, lanes),
                    turned_ref[i * 3 + j],
                    preferred_element_type=jnp.float32,
                )
                grad_act = term if grad_act is None else grad_act + term
        rows = pl.ds(n * count, count)
        normed, inv_rms, unit = normalised(features_ref[rows].astype(jnp.float32), gain)
        sigma = 1.0 / (1.0 + jnp.exp(-normed))
        grad_unit = grad_act * sigma * (1.0 + normed * (1.0 - sigma)) * gain
        mean = jnp.mean(grad_unit * unit, axis=-1, keepdims=True)
        out_ref[rows] = (inv_rms * (grad_unit - unit * mean)).astype(jnp.bfloat16)
        return carry

    lax.fori_loop(0, (frames - 2) // step, piece, 0)


def sum_first_kernel(blocks_ref, after_ref, out_ref):
    total = blocks_ref[0].astype(jnp.float32)
    for p in range(1, blocks_ref.shape[0]):
        total = total + blocks_ref[p].astype(jnp.float32)
    if len(out_ref.shape) == 2:
        out_ref[...] = total
    else:
        for p in range(out_ref.shape[0]):
            out_ref[p] = total


def sum_last_kernel(scale, blocks_ref, out_ref):
    total = blocks_ref[0]
    for p in range(1, blocks_ref.shape[0]):
        total = total + blocks_ref[p]
    total = (total * scale).astype(jnp.bfloat16)
    for p in range(out_ref.shape[0]):
        out_ref[p] = total


def unpack_kernel(rows, columns, core_ref, blocks_ref, *refs):
    owner = core_ref[0]
    out_ref, whole_ref, sem, last_sem = refs[-4:]
    full, rest, strips, per_tile, extra = tile_plan(rows, columns)
    outputs = out_ref.shape[2]
    taps = columns // outputs
    pairs, middle = tap_plan()
    groups = blocks_ref.shape[0]
    common = taps - 1

    def copy_of(g):
        here = pl.ds(g * rows, rows)
        return pltpu.make_async_copy(
            whole_ref.at[pl.ds(0, common), here],
            out_ref.at[pl.ds(owner * taps, common), here],
            sem.at[g],
        )

    def last_copy():
        return pltpu.make_async_copy(
            whole_ref.at[pl.ds(common, 1)], out_ref.at[pl.ds(common, 1)], last_sem
        )

    for g in range(groups):
        block = blocks_ref[g].astype(jnp.float32)

        def tile(n):
            return block[n * SUBLANES : (n + 1) * SUBLANES]

        spans = [
            jnp.concatenate([tile(s * full + t) for s in range(strips)], axis=0)
            for t in range(full)
        ]
        if rest:
            ends = []
            for s in range(strips):
                at = (s % per_tile) * rest
                ends.append(tile(strips * full + s // per_tile)[:, at : at + rest])
            spans.append(jnp.concatenate(ends, axis=0))
        for t in range(taps):
            if t < 3 * pairs:
                at = t + owner
            else:
                at = t - owner * t
            begin, end = t * outputs, (t + 1) * outputs
            parts = []
            while begin < end:
                n, low = divmod(begin, LANES)
                high = min(LANES, low + end - begin)
                parts.append(spans[n][:, low:high])
                begin += high - low
            whole_ref[at, g * rows : (g + 1) * rows] = jnp.concatenate(parts, axis=-1)
        copy_of(g).start()

    @pl.when(owner == 0)
    def _():
        last = last_copy()
        last.start()
        last.wait()

    for g in range(groups):
        copy_of(g).wait()


def exchange(blocks, axis):
    return lax.all_to_all(blocks, axis, 0, 0, tiled=True)


def on_device(features, norm_gain, conv_weight, out_grad):
    frames, height, width, channels = features.shape
    outputs = out_grad.shape[3]
    count = frames * height * width
    groups, far, near, cores = (lax.axis_size(a) for a in ("tm", *ROWS))
    chips = far * near
    core = lax.axis_index("core")
    core_arg = core.astype(jnp.int32).reshape(1)
    swap = [(0, 1), (1, 0)]

    later = 2
    block_of = functools.partial(jax.ShapeDtypeStruct, dtype=jnp.bfloat16)
    flat = features.reshape(count, channels)
    gain = norm_gain.reshape(1, channels)
    rows_own, head, edge, corner, act = pl.pallas_call(
        split_kernel,
        out_shape=(
            block_of((height, frames, width, outputs)),
            block_of((later, height, width, outputs)),
            block_of((frames, width, outputs)),
            block_of((later, width, outputs)),
            block_of((frames, channels, height * width)),
        ),
        in_specs=[smem()] + [anywhere()] * 3,
        out_specs=(vmem(),) * 5,
        scratch_shapes=[
            pltpu.VMEM(out_grad.shape, jnp.bfloat16),
            pltpu.VMEM((count, channels), jnp.bfloat16),
            pltpu.VMEM((1, channels), jnp.float32),
            pltpu.SemaphoreType.DMA((3,)),
        ],
        cost_estimate=cost(count * channels * 20, count * (outputs + channels) * 4),
        compiler_params=GRANT,
        name="split",
    )(
        core_arg,
        *(pltpu.with_memory_space_constraint(a, pltpu.HBM) for a in (out_grad, flat, gain)),
    )
    across = [(2 * z + 1, 2 * z + 2) for z in range(chips - 1)]
    across += [(b, a) for a, b in across]
    lines = 2 * chips
    slanted = [
        ((g + 1) * lines + a, g * lines + b) for g in range(groups - 1) for a, b in across
    ]
    after = lax.ppermute(head, "tm", [(g + 1, g) for g in range(groups - 1)])
    outer = lax.ppermute(edge, ROWS, across)
    outer_after = lax.ppermute(corner, ("tm", *ROWS), slanted)
    _, first_row = packet_plan(frames, channels, width)
    length = first_row + (frames + later) * (height + 1)
    packet = pl.pallas_call(
        merge_kernel,
        out_shape=jax.ShapeDtypeStruct((length, width, LANES), jnp.bfloat16),
        in_specs=[vmem()] * 5,
        out_specs=vmem(),
        cost_estimate=cost(1000, count * channels * 4),
        compiler_params=GRANT,
        name="merge",
    )(act, rows_own, after, outer, outer_after)
    theirs = lax.ppermute(packet, "core", swap)

    pairs, middle = tap_plan()
    taps = 3 * pairs + middle
    columns = taps * outputs
    rows = channels // groups
    full, _, strips, _, extra = tile_plan(rows, columns)
    share = -(-(full * strips + extra) // chips) * SUBLANES
    token = jax.ShapeDtypeStruct((SUBLANES, LANES), jnp.float32)
    terms, inner = pl.pallas_call(
        kernel_grad_kernel,
        out_shape=(
            jax.ShapeDtypeStruct((groups, chips * share, LANES), jnp.bfloat16),
            block_of((frames + later, width, outputs)),
        ),
        in_specs=[smem()] + [vmem()] * 2,
        out_specs=(vmem(), vmem()),
        scratch_shapes=[
            pltpu.VMEM((frames + 2, 2 * (height + 1), width, 3 * LANES), jnp.bfloat16),
            pltpu.VMEM((channels, columns), jnp.float32),
            pltpu.VMEM((frames + 2, width + 2 * SUBLANES, LANES), jnp.float32),
        ],
        cost_estimate=cost(2 * 2 * count * channels * columns, 2 * channels * columns),
        compiler_params=GRANT,
        name="kernel_grad",
    )(core_arg, packet, theirs)

    grad_features, features_done = pl.pallas_call(
        features_kernel,
        out_shape=(jax.ShapeDtypeStruct((count, channels), jnp.bfloat16), token),
        in_specs=[smem()] + [vmem()] * 5,
        out_specs=(vmem(), vmem()),
        scratch_shapes=[
            pltpu.VMEM((frames + 2, height + 2, width, 3 * outputs), jnp.bfloat16),
            pltpu.VMEM((9, 3 * outputs, channels), jnp.bfloat16),
        ],
        cost_estimate=cost(2 * count * channels * 27 * outputs, 2 * 27 * channels * outputs),
        compiler_params=GRANT,
        name="grad_features",
    )(
        core_arg,
        packet,
        inner,
        flat,
        gain,
        conv_weight.reshape(27, channels, outputs),
    )

    first = ("tm", "near")
    peers = groups * near
    block = far * share
    received = exchange(terms.reshape(peers, block, LANES), first)
    summed = pl.pallas_call(
        sum_first_kernel,
        out_shape=jax.ShapeDtypeStruct(
            (far, block, LANES) if ONE_STAGE else (block, LANES), jnp.float32
        ),
        in_specs=[vmem(), anywhere()],
        out_specs=vmem(),
        cost_estimate=cost(count * channels, 2 * channels * columns),
        compiler_params=GRANT,
        name="sum_first",
    )(received, features_done)
    part = block if ONE_STAGE else share
    received = exchange(summed.reshape(far, part, LANES), "far")
    positions = count * groups * chips * cores
    scale = float(positions) ** -0.5
    total = pl.pallas_call(
        functools.partial(sum_last_kernel, scale),
        out_shape=jax.ShapeDtypeStruct((peers if ONE_STAGE else far, part, LANES), jnp.bfloat16),
        in_specs=[vmem()],
        out_specs=vmem(),
        cost_estimate=cost(count * channels, 8 * far * part * LANES),
        compiler_params=GRANT,
        name="sum_last",
    )(received)
    if not ONE_STAGE:
        gathered = exchange(total, "far").reshape(1, block, LANES)
        total = jnp.broadcast_to(gathered, (peers, block, LANES))
    gathered = exchange(total, first).reshape(groups, chips * share, LANES)
    gathered_theirs = lax.ppermute(gathered, "core", swap)
    whole = jax.ShapeDtypeStruct((27, channels, outputs), jnp.float32)

    def unpack(owner, blocks, *so_far):
        return pl.pallas_call(
            functools.partial(unpack_kernel, rows, columns),
            out_shape=whole,
            in_specs=[smem(), vmem()] + [anywhere() for _ in so_far],
            out_specs=anywhere(),
            scratch_shapes=[
                pltpu.VMEM((taps, channels, outputs), jnp.float32),
                pltpu.SemaphoreType.DMA((groups,)),
                pltpu.SemaphoreType.DMA,
            ],
            input_output_aliases={2: 0} if so_far else {},
            cost_estimate=cost(27 * channels * outputs * 8, 4 * 27 * channels * outputs),
            compiler_params=GRANT,
            name="unpack",
        )(owner, blocks, *so_far)

    grad_weight = unpack(core_arg, gathered)
    grad_weight = unpack(1 - core_arg, gathered_theirs, grad_weight)
    return (
        grad_features.reshape(features.shape),
        grad_weight.reshape(3, 3, 3, channels, outputs),
    )


def solution(mesh):
    clips, groups, lines = (mesh.shape[a] for a in ("clips", "tm", "rows"))
    torus = Mesh(
        mesh.devices.reshape(clips, groups, lines // (2 * NEAR), NEAR, 2), ("clips", "tm", *ROWS)
    )
    in_specs = (
        P(("clips", "tm"), ROWS, None, None),
        P(),
        P(),
        P(("clips", "tm"), ROWS, None, None),
    )
    out_specs = (P(("clips", "tm"), ROWS, None, None), P("clips", None, None, None, None))
    return jax.shard_map(
        on_device, mesh=torus, in_specs=in_specs, out_specs=out_specs, check_vma=False
    )
```

```python
import functools

import jax
import jax.numpy as jnp
from jax import lax
from jax.experimental import pallas as pl
from jax.experimental.pallas import tpu as pltpu
from jax.sharding import Mesh
from jax.sharding import PartitionSpec as P

NEAR = 4
ONE_STAGE = True
ROWS = ("far", "near", "core")
LANES = 128
SUBLANES = 8
GRANT = pltpu.CompilerParams(vmem_limit_bytes=20 * 2**20)


def vmem():
    return pl.BlockSpec(memory_space=pltpu.VMEM)


def smem():
    return pl.BlockSpec(memory_space=pltpu.SMEM)


def anywhere():
    return pl.BlockSpec(memory_space=pl.ANY)


def cost(flops, moved):
    return pl.CostEstimate(flops=flops, bytes_accessed=moved, transcendentals=0)


def normalised(values, gain):
    inv_rms = lax.rsqrt(jnp.mean(values * values, axis=-1, keepdims=True) + 1e-06)
    unit = values * inv_rms
    return unit * gain, inv_rms, unit


def split_kernel(core_ref, out_grad_hbm, rows_ref, head_ref, edge_ref, out_grad_ref, sem):
    fetch = pltpu.make_async_copy(out_grad_hbm, out_grad_ref, sem)
    fetch.start()
    fetch.wait()
    height = rows_ref.shape[0]
    for r in range(height):
        rows_ref[r] = out_grad_ref[:, r]
    head_ref[...] = out_grad_ref[: head_ref.shape[0]]
    edge_ref[...] = out_grad_ref[:, core_ref[0] * (height - 1)]


def act_kernel(features_hbm, gain_hbm, act_ref, features_ref, gain_ref, sem):
    fetches = [
        pltpu.make_async_copy(features_hbm, features_ref, sem.at[0]),
        pltpu.make_async_copy(gain_hbm, gain_ref, sem.at[1]),
    ]
    for fetch in fetches:
        fetch.start()
    for fetch in fetches:
        fetch.wait()
    normed, _, _ = normalised(features_ref[...].astype(jnp.float32), gain_ref[...])
    act = (normed / (1.0 + jnp.exp(-normed))).T.astype(jnp.bfloat16)
    frames = act_ref.shape[0]
    positions = act.shape[1] // frames
    for t in range(frames):
        act_ref[t] = act[:, t * positions : (t + 1) * positions]


def packet_plan(frames, channels, width):
    per_frame = channels // width
    return per_frame, per_frame * frames


def merge_kernel(act_ref, rows_ref, after_ref, outer_ref, packet_ref):
    frames, channels, lanes = act_ref.shape
    height, _, width, outputs = rows_ref.shape
    _, first = packet_plan(frames, channels, width)
    later = after_ref.shape[0]
    packet_ref[:first] = act_ref[...].reshape(first, width, lanes)
    for r in range(height):
        at = first + r * (frames + later)
        packet_ref[at : at + frames, :, :outputs] = rows_ref[r]
        packet_ref[at + frames : at + frames + later, :, :outputs] = after_ref[:, r]
    at = first + height * (frames + later)
    packet_ref[at : at + frames, :, :outputs] = outer_ref[...]
    packet_ref[at + frames : at + frames + later, :, :outputs] = after_ref[:, height]


def packet_act(packet_ref, frames, channels):
    width, lanes = packet_ref.shape[1:]
    per_frame, first = packet_plan(frames, channels, width)
    blocks = [
        packet_ref[t * per_frame : (t + 1) * per_frame].reshape(channels, lanes)
        for t in range(frames)
    ]
    return jnp.concatenate(blocks, axis=-1)


def packet_row(packet_ref, row, frames, channels, outputs):
    width = packet_ref.shape[1]
    _, first = packet_plan(frames, channels, width)
    return packet_ref[pl.ds(first + row * (frames + 2), frames + 2), :, :outputs]


def column_taps(block):
    block = block.astype(jnp.float32)
    axis = block.ndim - 2
    width = block.shape[axis]
    column = lax.broadcasted_iota(jnp.int32, block.shape, axis)
    later = jnp.where(column == width - 1, 0.0, pltpu.roll(block, width - 1, axis))
    sooner = jnp.where(column == 0, 0.0, pltpu.roll(block, 1, axis))
    return jnp.concatenate([later, block, sooner], axis=-1).astype(jnp.bfloat16)


def tap_plan():
    return 4, 2


def tile_plan(rows, columns):
    full, rest = divmod(columns, LANES)
    strips = rows // SUBLANES
    per_tile = LANES // rest if rest else 1
    extra = -(-strips // per_tile) if rest else 0
    return full, rest, strips, per_tile, extra


def kernel_grad_kernel(
    core_ref,
    mine_ref,
    theirs_ref,
    out_ref,
    inner_ref,
    taps_ref,
    terms_ref,
    shift_ref,
):
    core = core_ref[0]
    other = 1 - core
    frames = taps_ref.shape[0]
    height = taps_ref.shape[1] // 2 - 1
    channels = terms_ref.shape[0]
    outputs = inner_ref.shape[2]
    inner_ref[...] = packet_row(theirs_ref, core * (height - 1), frames - 2, channels, outputs)

    width = taps_ref.shape[2]
    pad = SUBLANES
    shift_ref[:, :pad] = jnp.zeros_like(shift_ref[:, :pad])
    shift_ref[:, pad + width :] = jnp.zeros_like(shift_ref[:, pad + width :])
    _, first = packet_plan(frames - 2, channels, width)

    def place_row(ref, row, slot):
        block = ref[pl.ds(first + row * frames, frames)]
        shift_ref[:, pad : pad + width] = block.astype(jnp.float32)
        taps_ref[:, slot, :, :LANES] = shift_ref[:, pad + 1 : pad + 1 + width].astype(jnp.bfloat16)
        taps_ref[:, slot, :, LANES : 2 * LANES] = block
        taps_ref[:, slot, :, 2 * LANES :] = shift_ref[:, pad - 1 : pad - 1 + width].astype(
            jnp.bfloat16
        )

    for ref, place in ((mine_ref, core), (theirs_ref, other)):
        for row in range(height):
            place_row(ref, row, place * height + row + 1)
        place_row(ref, height, place * (2 * height + 1))
    act = packet_act(mine_ref, frames - 2, channels)
    act_theirs = packet_act(theirs_ref, frames - 2, channels)
    lanes = taps_ref.shape[3]
    positions = act.shape[1]
    pairs, middle = tap_plan()

    def pair(i, j):
        total = None
        for left, place in ((act, core), (act_theirs, other)):
            shifted = taps_ref[pl.ds(2 - i, frames - 2), pl.ds(place * height + 2 - j, height)]
            term = jnp.dot(
                left, shifted.reshape(positions, lanes), preferred_element_type=jnp.float32
            )
            total = term if total is None else total + term
        return total

    def keep(tap, total, k):
        terms_ref[:, tap * outputs : (tap + 1) * outputs] = total[:, k * LANES : k * LANES + outputs]

    for n in range(pairs):
        p = core * (pairs + 1) + n
        total = pair(p // 3, p % 3)
        for k in range(3):
            keep(3 * n + k, total, k)
    centre = pair(1, 1)
    centre = jnp.where(
        core == 0, centre[:, : middle * LANES], centre[:, lanes - middle * LANES :]
    )
    for k in range(middle):
        keep(3 * pairs + k, centre, k)

    groups, packed, _ = out_ref.shape
    rows = act.shape[0] // groups
    full, rest, strips, per_tile, extra = tile_plan(rows, terms_ref.shape[1])
    zeros = jnp.zeros((SUBLANES, LANES), jnp.float32)
    for g in range(groups):

        def strip(s, span):
            at = g * rows + s * SUBLANES
            return terms_ref[at : at + SUBLANES, span]

        tiles = [
            strip(s, slice(t * LANES, (t + 1) * LANES)) for s in range(strips) for t in range(full)
        ]
        for e in range(extra):
            ends = [
                strip(s, slice(full * LANES, full * LANES + rest))
                for s in range(e * per_tile, min((e + 1) * per_tile, strips))
            ]
            used = rest * len(ends)
            if used < LANES:
                ends.append(zeros[:, used:])
            tiles.append(jnp.concatenate(ends, axis=-1))
        tiles += [zeros] * (packed // SUBLANES - len(tiles))
        out_ref[g] = jnp.concatenate(tiles, axis=0).astype(jnp.bfloat16)


def features_kernel(
    core_ref,
    mine_ref,
    inner_ref,
    features_ref,
    gain_ref,
    weight_ref,
    out_ref,
    token_ref,
    taps_ref,
    turned_ref,
):
    core = core_ref[0]
    frames, height, width = taps_ref.shape[:3]
    height = height - 2
    outputs = inner_ref.shape[2]
    channels = features_ref.shape[1]
    token_ref[...] = jnp.zeros_like(token_ref)

    def row_of(ref, row):
        return column_taps(packet_row(ref, row, frames - 2, channels, outputs))

    def build(row, carry):
        taps_ref[:, row + 1] = row_of(mine_ref, row)
        return carry

    lax.fori_loop(0, height, build, 0)
    taps_ref[:, core * (height + 1)] = row_of(mine_ref, height)
    taps_ref[:, (1 - core) * (height + 1)] = column_taps(inner_ref[...])

    def turn(n, carry):
        for k in range(3):
            turned = weight_ref[n * 3 + k].astype(jnp.float32).T
            turned_ref[n, k * outputs : (k + 1) * outputs] = turned.astype(jnp.bfloat16)
        return carry

    lax.fori_loop(0, 9, turn, 0)
    gain = gain_ref[...]
    lanes = taps_ref.shape[3]
    step = 2
    count = step * height * width

    def piece(n, carry):
        grad_act = None
        for i in range(3):
            for j in range(3):
                shifted = taps_ref[pl.ds(n * step + 2 - i, step), 2 - j : 2 - j + height]
                term = jnp.dot(
                    shifted.reshape(count, lanes),
                    turned_ref[i * 3 + j],
                    preferred_element_type=jnp.float32,
                )
                grad_act = term if grad_act is None else grad_act + term
        rows = pl.ds(n * count, count)
        normed, inv_rms, unit = normalised(features_ref[rows].astype(jnp.float32), gain)
        sigma = 1.0 / (1.0 + jnp.exp(-normed))
        grad_unit = grad_act * sigma * (1.0 + normed * (1.0 - sigma)) * gain
        mean = jnp.mean(grad_unit * unit, axis=-1, keepdims=True)
        out_ref[rows] = (inv_rms * (grad_unit - unit * mean)).astype(jnp.bfloat16)
        return carry

    lax.fori_loop(0, (frames - 2) // step, piece, 0)


def sum_first_kernel(blocks_ref, after_ref, out_ref):
    total = blocks_ref[0].astype(jnp.float32)
    for p in range(1, blocks_ref.shape[0]):
        total = total + blocks_ref[p].astype(jnp.float32)
    if len(out_ref.shape) == 2:
        out_ref[...] = total
    else:
        for p in range(out_ref.shape[0]):
            out_ref[p] = total


def sum_last_kernel(scale, blocks_ref, out_ref):
    total = blocks_ref[0]
    for p in range(1, blocks_ref.shape[0]):
        total = total + blocks_ref[p]
    total = (total * scale).astype(jnp.bfloat16)
    for p in range(out_ref.shape[0]):
        out_ref[p] = total


def unpack_kernel(rows, columns, core_ref, blocks_ref, *refs):
    owner = core_ref[0]
    out_ref, whole_ref, sem, last_sem = refs[-4:]
    full, rest, strips, per_tile, extra = tile_plan(rows, columns)
    outputs = out_ref.shape[2]
    taps = columns // outputs
    pairs, middle = tap_plan()
    groups = blocks_ref.shape[0]
    common = taps - 1

    def copy_of(g):
        here = pl.ds(g * rows, rows)
        return pltpu.make_async_copy(
            whole_ref.at[pl.ds(0, common), here],
            out_ref.at[pl.ds(owner * taps, common), here],
            sem.at[g],
        )

    def last_copy():
        return pltpu.make_async_copy(
            whole_ref.at[pl.ds(common, 1)], out_ref.at[pl.ds(common, 1)], last_sem
        )

    for g in range(groups):
        block = blocks_ref[g].astype(jnp.float32)

        def tile(n):
            return block[n * SUBLANES : (n + 1) * SUBLANES]

        spans = [
            jnp.concatenate([tile(s * full + t) for s in range(strips)], axis=0)
            for t in range(full)
        ]
        if rest:
            ends = []
            for s in range(strips):
                at = (s % per_tile) * rest
                ends.append(tile(strips * full + s // per_tile)[:, at : at + rest])
            spans.append(jnp.concatenate(ends, axis=0))
        for t in range(taps):
            if t < 3 * pairs:
                at = t + owner
            else:
                at = t - owner * t
            begin, end = t * outputs, (t + 1) * outputs
            parts = []
            while begin < end:
                n, low = divmod(begin, LANES)
                high = min(LANES, low + end - begin)
                parts.append(spans[n][:, low:high])
                begin += high - low
            whole_ref[at, g * rows : (g + 1) * rows] = jnp.concatenate(parts, axis=-1)
        copy_of(g).start()

    @pl.when(owner == 0)
    def _():
        last = last_copy()
        last.start()
        last.wait()

    for g in range(groups):
        copy_of(g).wait()


def exchange(blocks, axis):
    return lax.all_to_all(blocks, axis, 0, 0, tiled=True)


def on_device(features, norm_gain, conv_weight, out_grad):
    frames, height, width, channels = features.shape
    outputs = out_grad.shape[3]
    count = frames * height * width
    groups, far, near, cores = (lax.axis_size(a) for a in ("tm", *ROWS))
    chips = far * near
    core = lax.axis_index("core")
    core_arg = core.astype(jnp.int32).reshape(1)
    swap = [(0, 1), (1, 0)]

    later = 2
    block_of = functools.partial(jax.ShapeDtypeStruct, dtype=jnp.bfloat16)
    flat = features.reshape(count, channels)
    gain = norm_gain.reshape(1, channels)
    out_grad_hbm, flat_hbm, gain_hbm = (
        pltpu.with_memory_space_constraint(a, pltpu.HBM) for a in (out_grad, flat, gain)
    )
    rows_own, head, edge = pl.pallas_call(
        split_kernel,
        out_shape=(
            block_of((height, frames, width, outputs)),
            block_of((later, height, width, outputs)),
            block_of((frames, width, outputs)),
        ),
        in_specs=[smem(), anywhere()],
        out_specs=(vmem(),) * 3,
        scratch_shapes=[pltpu.VMEM(out_grad.shape, jnp.bfloat16), pltpu.SemaphoreType.DMA],
        cost_estimate=cost(1000, count * outputs * 4),
        compiler_params=GRANT,
        name="split",
    )(core_arg, out_grad_hbm)
    act = pl.pallas_call(
        act_kernel,
        out_shape=block_of((frames, channels, height * width)),
        in_specs=[anywhere()] * 2,
        out_specs=vmem(),
        scratch_shapes=[
            pltpu.VMEM((count, channels), jnp.bfloat16),
            pltpu.VMEM((1, channels), jnp.float32),
            pltpu.SemaphoreType.DMA((2,)),
        ],
        cost_estimate=cost(count * channels * 20, count * channels * 4),
        compiler_params=GRANT,
        name="act",
    )(flat_hbm, gain_hbm)
    across = [(2 * z + 1, 2 * z + 2) for z in range(chips - 1)]
    across += [(b, a) for a, b in across]
    outer = lax.ppermute(edge, ROWS, across)
    head = jnp.concatenate([head, outer[:later, None]], axis=1)
    after = lax.ppermute(head, "tm", [(g + 1, g) for g in range(groups - 1)])
    _, first_row = packet_plan(frames, channels, width)
    length = first_row + (frames + later) * (height + 1)
    packet = pl.pallas_call(
        merge_kernel,
        out_shape=jax.ShapeDtypeStruct((length, width, LANES), jnp.bfloat16),
        in_specs=[vmem()] * 4,
        out_specs=vmem(),
        cost_estimate=cost(1000, count * channels * 4),
        compiler_params=GRANT,
        name="merge",
    )(act, rows_own, after, outer)
    theirs = lax.ppermute(packet, "core", swap)

    pairs, middle = tap_plan()
    taps = 3 * pairs + middle
    columns = taps * outputs
    rows = channels // groups
    full, _, strips, _, extra = tile_plan(rows, columns)
    share = -(-(full * strips + extra) // chips) * SUBLANES
    token = jax.ShapeDtypeStruct((SUBLANES, LANES), jnp.float32)
    terms, inner = pl.pallas_call(
        kernel_grad_kernel,
        out_shape=(
            jax.ShapeDtypeStruct((groups, chips * share, LANES), jnp.bfloat16),
            block_of((frames + later, width, outputs)),
        ),
        in_specs=[smem()] + [vmem()] * 2,
        out_specs=(vmem(), vmem()),
        scratch_shapes=[
            pltpu.VMEM((frames + 2, 2 * (height + 1), width, 3 * LANES), jnp.bfloat16),
            pltpu.VMEM((channels, columns), jnp.float32),
            pltpu.VMEM((frames + 2, width + 2 * SUBLANES, LANES), jnp.float32),
        ],
        cost_estimate=cost(2 * 2 * count * channels * columns, 2 * channels * columns),
        compiler_params=GRANT,
        name="kernel_grad",
    )(core_arg, packet, theirs)

    grad_features, features_done = pl.pallas_call(
        features_kernel,
        out_shape=(jax.ShapeDtypeStruct((count, channels), jnp.bfloat16), token),
        in_specs=[smem()] + [vmem()] * 5,
        out_specs=(vmem(), vmem()),
        scratch_shapes=[
            pltpu.VMEM((frames + 2, height + 2, width, 3 * outputs), jnp.bfloat16),
            pltpu.VMEM((9, 3 * outputs, channels), jnp.bfloat16),
        ],
        cost_estimate=cost(2 * count * channels * 27 * outputs, 2 * 27 * channels * outputs),
        compiler_params=GRANT,
        name="grad_features",
    )(
        core_arg,
        packet,
        inner,
        flat,
        gain,
        conv_weight.reshape(27, channels, outputs),
    )

    first = ("tm", "near")
    peers = groups * near
    block = far * share
    received = exchange(terms.reshape(peers, block, LANES), first)
    summed = pl.pallas_call(
        sum_first_kernel,
        out_shape=jax.ShapeDtypeStruct(
            (far, block, LANES) if ONE_STAGE else (block, LANES), jnp.float32
        ),
        in_specs=[vmem(), anywhere()],
        out_specs=vmem(),
        cost_estimate=cost(count * channels, 2 * channels * columns),
        compiler_params=GRANT,
        name="sum_first",
    )(received, features_done)
    part = block if ONE_STAGE else share
    received = exchange(summed.reshape(far, part, LANES), "far")
    positions = count * groups * chips * cores
    scale = float(positions) ** -0.5
    total = pl.pallas_call(
        functools.partial(sum_last_kernel, scale),
        out_shape=jax.ShapeDtypeStruct((peers if ONE_STAGE else far, part, LANES), jnp.bfloat16),
        in_specs=[vmem()],
        out_specs=vmem(),
        cost_estimate=cost(count * channels, 8 * far * part * LANES),
        compiler_params=GRANT,
        name="sum_last",
    )(received)
    if not ONE_STAGE:
        gathered = exchange(total, "far").reshape(1, block, LANES)
        total = jnp.broadcast_to(gathered, (peers, block, LANES))
    gathered = exchange(total, first).reshape(groups, chips * share, LANES)
    gathered_theirs = lax.ppermute(gathered, "core", swap)
    whole = jax.ShapeDtypeStruct((27, channels, outputs), jnp.float32)

    def unpack(owner, blocks, *so_far):
        return pl.pallas_call(
            functools.partial(unpack_kernel, rows, columns),
            out_shape=whole,
            in_specs=[smem(), vmem()] + [anywhere() for _ in so_far],
            out_specs=anywhere(),
            scratch_shapes=[
                pltpu.VMEM((taps, channels, outputs), jnp.float32),
                pltpu.SemaphoreType.DMA((groups,)),
                pltpu.SemaphoreType.DMA,
            ],
            input_output_aliases={2: 0} if so_far else {},
            cost_estimate=cost(27 * channels * outputs * 8, 4 * 27 * channels * outputs),
            compiler_params=GRANT,
            name="unpack",
        )(owner, blocks, *so_far)

    grad_weight = unpack(core_arg, gathered)
    grad_weight = unpack(1 - core_arg, gathered_theirs, grad_weight)
    return (
        grad_features.reshape(features.shape),
        grad_weight.reshape(3, 3, 3, channels, outputs),
    )


def solution(mesh):
    clips, groups, lines = (mesh.shape[a] for a in ("clips", "tm", "rows"))
    torus = Mesh(
        mesh.devices.reshape(clips, groups, lines // (2 * NEAR), NEAR, 2), ("clips", "tm", *ROWS)
    )
    in_specs = (
        P(("clips", "tm"), ROWS, None, None),
        P(),
        P(),
        P(("clips", "tm"), ROWS, None, None),
    )
    out_specs = (P(("clips", "tm"), ROWS, None, None), P("clips", None, None, None, None))
    return jax.shard_map(
        on_device, mesh=torus, in_specs=in_specs, out_specs=out_specs, check_vma=False
    )
```
